256 devices in a mesh: section: 4 (over y), node: 8 (over z), torus: 8 (over x, core).
Axes of the slice: x: 4, y: 4, z: 8, core: 2. Of those that a mesh axis runs over, the one named last changes fastest.
Arguments:
- act_in: bfloat16 [4, 2048, 7168], P('section', 'node', 'torus'), may hold values from -28 to 28
- next_in: bfloat16 [2048, 7168], P('node', 'torus'), may hold values from -42 to 42
- routes: int32 [2, 4, 2048, 2], P(None, 'section', 'node'), may hold values from 0 to 7, all different within a row; in each aligned block of 256 rows (0 to 255, 256 to 511, ..., all dimensions but the last counted through in order) at most 80 rows name the same one
- route_w: float32 [2, 4, 2048, 2], P(None, 'section', 'node'), may hold values from 0.2 to 1
- hist: float32 [4], P('section'), may hold values from 2 to 8
- gate_w: bfloat16 [4, 8, 7168, 1024], P('section', 'node', 'torus'), may hold values from -0.0625 to 0.0625
- up_w: bfloat16 [4, 8, 7168, 1024], P('section', 'node', 'torus'), may hold values from -0.0625 to 0.0625
- down_w: bfloat16 [4, 8, 1024, 7168], P('section', 'node', None, 'torus'), may hold values from -0.09375 to 0.09375
Outputs:
- act_out: bfloat16 [2, 4, 2048, 7168], P(None, 'section', 'node', 'torus')
- peak_out: float32 [4, 2], P('section')
The draws below stay inside these ranges and needn't reach their ends.
Inputs may be any that keep to these rules, and one draw needn't show every extreme that they name: `routes`: each token names 2 different experts; within the 256 tokens of one index of node (aligned blocks of rows of one tick and layer) no expert is named more than 80 times, a bound that some block reaches.
All inputs are finite; a program needn't handle non-finite values.
Results may differ from the reference program's by a relative error of at most 0.012.
Values may be sent and summed in bfloat16 or wider, within the bound.
A program may use at most 64 MiB of HBM per device.

```python
import math
import jax
import jax.numpy as jnp
import numpy as np
from jax import lax

D = 7168
FFW = 1024
TOPK = 2
TICKS = 2
TOK_DEV = 256
SECTIONS = 4
EXPERTS = 8
CAP = 80
TOKENS = 2048
N_NODE = 8


def rising_rows(key, array_shape, factor):
    noise_key, scale_key = jax.random.split(key)
    rising = 1.0 + 2.0 * jnp.arange(TOKENS, dtype=jnp.float32) / TOKENS
    noise = jnp.clip(jax.random.normal(noise_key, array_shape, jnp.float32), -6.0, 6.0)
    spread = jnp.exp(jax.random.uniform(scale_key, array_shape[:-1] + (1,), jnp.float32, -0.7, 0.4))
    return (noise * spread * rising[:, None] * factor).astype(jnp.bfloat16)


def draw_act_in(key, part):
    return rising_rows(jax.random.fold_in(key, 11), (SECTIONS, TOKENS, D), 1.0)


def draw_next_in(key, part):
    return rising_rows(jax.random.fold_in(key, 23), (TOKENS, D), 1.5)


def levels(stream_key, dims, shards, low, top_value):
    level, own = 1.0, jax.random.fold_in(stream_key, 6)
    for axis_at, blocks in shards:
        steps = jnp.exp(jax.random.uniform(jax.random.fold_in(own, axis_at), (blocks,), jnp.float32, low / len(shards), top_value / len(shards)))
        level = level * jnp.repeat(steps, dims[axis_at] // blocks).reshape([-1 if axis == axis_at else 1 for axis in range(len(dims))])
    return level


def routed_block(own_key, own, number, rows, amount, top, reach, lean):
    order = jax.random.permutation(own_key, amount)
    heavy_load, ordinary = shares(amount, rows * top, reach, lean, True), shares(amount, rows * top, reach, lean, False)
    places = jnp.arange(amount)

    def named(tallies, turn):
        used = int((tallies > 0).sum())
        fixed = max(1, used // 4)
        shifted = fixed + (places - fixed + turn * (used - fixed)) % max(1, amount - fixed)
        return jnp.zeros((amount,), jnp.int32).at[order[jnp.where(places < fixed, places, shifted)]].set(jnp.asarray(tallies, jnp.int32))

    tallies = jnp.where(number % 4 == 0, named(heavy_load, number // 4), named(ordinary, number - number // 4 - 1))
    mixed = jax.random.permutation(jax.random.fold_in(own, 3), amount)
    source_of, sink = mixed[0:amount // 2 * 2:2], mixed[1:amount // 2 * 2:2]
    slack = jnp.minimum(tallies[source_of] - 1, reach - tallies[sink]) // 2
    slack = jnp.where((source_of == order[0]) | (sink == order[0]) | (tallies[sink] == 0), 0, jnp.maximum(slack, 0))
    shifted = jax.random.randint(jax.random.fold_in(own, 4), (amount // 2,), 0, 1 << 20) % (slack + 1)
    tallies = tallies.at[source_of].add(-shifted).at[sink].add(shifted)
    members = jnp.searchsorted(jnp.cumsum(tallies), jnp.arange(rows * top), side="right").astype(jnp.int32)
    grid = members.reshape(top, rows).T
    grid = grid[jax.random.permutation(jax.random.fold_in(own, 1), rows)]
    turn = jax.random.randint(jax.random.fold_in(own, 2), (rows, 1), 0, top)
    return jnp.take_along_axis(grid, (jnp.arange(top)[None, :] + turn) % top, axis=1)


def shares(count, total, limit, lean, full):
    portions = [(1 << 20) // math.isqrt(rank ** lean) + 1 for rank in range(1, count + 1)]
    largest = limit if full else min(limit, max(-(-total // count), total * portions[0] // sum(portions)))
    least = 1 if total - largest >= count - 1 else 0
    given, surplus = [largest] + [least] * (count - 1), total - largest - least * (count - 1)
    while surplus > 0:
        free = [i for i in range(1, count) if given[i] < largest] or [i for i in range(1, count) if given[i] < limit]
        pool, remaining = sum([portions[i] for i in free]), surplus
        for i in free:
            more = min(limit - given[i], max(1, remaining * portions[i] // pool), surplus)
            given[i] = given[i] + more
            surplus = surplus - more
    return np.array(given)


def bell_draw(stream_key, extent, scale, reach, cuts=(), held_as=jnp.bfloat16):
    values = scale * jax.random.normal(stream_key, extent, jnp.float32)
    if cuts:
        values = values * levels(stream_key, extent, cuts, -0.22, 0.18)
    return jnp.clip(values, -reach, reach).astype(held_as)


def setup_inputs(seed: int = 0) -> dict:
    key_of = jax.random.split(jax.random.key(seed), 9)
    act_in = draw_act_in(jax.random.fold_in(key_of[8], 71), 0)
    next_in = draw_next_in(jax.random.fold_in(key_of[8], 71), 0)
    routes_keys = jax.random.split(jax.random.fold_in(key_of[2], 1), TICKS * SECTIONS * TOKENS // TOK_DEV)
    routes_turns = jax.random.permutation(jax.random.fold_in(key_of[2], 3), TICKS * SECTIONS * TOKENS // TOK_DEV)
    routes = jax.vmap(lambda own, number: routed_block(jax.random.fold_in(key_of[2], 2), own, number, TOK_DEV, EXPERTS, TOPK, CAP, 2))(routes_keys, routes_turns).reshape((TICKS, SECTIONS, TOKENS, TOPK))
    route_w = jnp.clip(0.2 + 0.8 * jax.random.uniform(key_of[3], (TICKS, SECTIONS, TOKENS, TOPK), jnp.float32) ** levels(key_of[3], (TICKS, SECTIONS, TOKENS, TOPK), ((1, 4), (2, 8)), -0.2, 0.2), 0.2, 1.0)
    hist = jnp.clip(2.0 + 6.0 * jax.random.uniform(key_of[4], (SECTIONS,), jnp.float32) ** levels(key_of[4], (SECTIONS,), ((0, 4),), -0.2, 0.2), 2.0, 8.0)
    gate_w = bell_draw(key_of[5], (SECTIONS, EXPERTS, D, FFW), D ** -0.5, 0.0625, ((0, 4), (1, 8), (2, 8)))
    up_w = bell_draw(key_of[6], (SECTIONS, EXPERTS, D, FFW), D ** -0.5, 0.0625, ((0, 4), (1, 8), (2, 8)))
    down_w = bell_draw(key_of[7], (SECTIONS, EXPERTS, FFW, D), (4 * FFW) ** -0.5, 0.09375, ((0, 4), (1, 8), (3, 8)))
    return dict(act_in=act_in, next_in=next_in, routes=routes, route_w=route_w, hist=hist, gate_w=gate_w, up_w=up_w, down_w=down_w)


FP8_LIMIT = 448.0


def expert_rows(token_rows, gate_mat, up_mat, down_mat, dequant):
    gate_val = jnp.dot(token_rows, gate_mat, preferred_element_type=jnp.float32) * dequant
    up_val = jnp.dot(token_rows, up_mat, preferred_element_type=jnp.float32) * dequant
    hidden = (jax.nn.silu(gate_val) * up_val).astype(jnp.bfloat16)
    return jnp.dot(hidden, down_mat, preferred_element_type=jnp.float32).astype(jnp.bfloat16)


def moe_layer(stream, quant_scale, expert_of, weight_of, gate_all, up_all, down_all):
    quantized = jnp.clip(stream.astype(jnp.float32) * (FP8_LIMIT / quant_scale), -FP8_LIMIT, FP8_LIMIT).astype(jnp.bfloat16)
    dequant = quant_scale / FP8_LIMIT
    pair_count = TOKENS * TOPK
    flat_expert = expert_of.reshape(pair_count).astype(jnp.int32)
    flat_weight = weight_of.reshape(pair_count)
    slot_total = N_NODE * CAP
    positions = jnp.arange(pair_count, dtype=jnp.int32)

    def per_expert(expert_id):
        sort_keys = jnp.where(flat_expert == expert_id, positions, pair_count)
        chosen = jnp.argsort(sort_keys, stable=True)[:slot_total].astype(jnp.int32)
        is_valid = (flat_expert[chosen] == expert_id).astype(jnp.float32)
        token_ids = chosen // TOPK
        token_rows = quantized[token_ids]
        outputs = expert_rows(token_rows, gate_all[expert_id], up_all[expert_id], down_all[expert_id], dequant)
        return token_ids, outputs.astype(jnp.float32) * (flat_weight[chosen] * is_valid)[:, None]

    token_ids, contrib = lax.map(per_expert, jnp.arange(EXPERTS, dtype=jnp.int32))
    branch = jnp.zeros((TOKENS, D), jnp.float32).at[token_ids.reshape(-1)].add(contrib.reshape(-1, D))
    return (stream.astype(jnp.float32) + branch).astype(jnp.bfloat16)


def reference(act_in, next_in, routes, route_w, hist, gate_w, up_w, down_w):
    first_peaks = []
    first_tick = []
    for section_id in range(SECTIONS):
        stream = act_in[section_id]
        first_peaks.append(jnp.max(jnp.abs(stream.astype(jnp.float32))))
        first_tick.append(moe_layer(stream, hist[section_id], routes[0, section_id], route_w[0, section_id], gate_w[section_id], up_w[section_id], down_w[section_id]))
    second_peaks = []
    second_tick = []
    for section_id in range(SECTIONS):
        stream = next_in if section_id == 0 else first_tick[section_id - 1]
        second_peaks.append(jnp.max(jnp.abs(stream.astype(jnp.float32))))
        second_tick.append(moe_layer(stream, first_peaks[section_id], routes[1, section_id], route_w[1, section_id], gate_w[section_id], up_w[section_id], down_w[section_id]))
    act_out = jnp.stack([jnp.stack(first_tick), jnp.stack(second_tick)])
    peak_out = jnp.stack([jnp.stack(first_peaks), jnp.stack(second_peaks)], axis=1)
    return act_out, peak_out
```

```python
import functools

import jax
import jax.numpy as jnp
from jax import lax
from jax.experimental import pallas as pl
from jax.experimental.pallas import tpu as pltpu
from jax.sharding import PartitionSpec as P

MESH = pl.DeviceIdType.MESH
FP8_LIMIT = 448.0
F32 = jnp.float32
BF16 = jnp.bfloat16


def source_tables(n_node):
    if n_node == 8:
        return ((0, 1, 6, 3), (7, 2, 5, 4))
    half = n_node // 2
    return (tuple(range(half)), tuple(range(half, n_node)))


def dot(a, b):
    return jnp.dot(a, b, preferred_element_type=F32)


def kernel(
    n_section, n_node, n_torus, capacity,
    act, nxt, lanes_e, rows_e, rows_w, hist, gate_hbm, up_hbm, down_hbm,
    out, peak_out,
    w_gate, w_up, w_down, quant, d_send, arrived, own_part, rs_send, rs_recv,
    hidden, r_send, results, combine_w, y_buf, pk_src, pk_node, pk_torus,
    s_w, s_wp, r_wp, s_d, r_d, s_rs, r_rs, s_h, r_h, s_r, r_r, s_y, r_y, s_pn, r_pn, s_pt, r_pt,
):
    ticks, tokens, width = out.shape
    n_x = n_torus // 2
    ffw = w_gate.shape[1]
    unit = ffw // n_x
    core_rel = source_tables(n_node)
    n_step = len(core_rel[0])
    where_rel = {rel: (c, k) for c in range(2) for k, rel in enumerate(core_rel[c])}

    sec = lax.axis_index("section")
    z = lax.axis_index("node")
    t = lax.axis_index("torus")
    x = t // 2
    c = t % 2
    mate = x * 2 + (1 - c)

    def rcopy(src, dst, ssem, rsem, node=None, torus=None, section=None):
        ids = {}
        if section is not None:
            ids["section"] = section
        if node is not None:
            ids["node"] = node
        if torus is not None:
            ids["torus"] = torus
        return pltpu.make_async_remote_copy(src, dst, ssem, rsem, device_id=ids, device_id_type=MESH)

    def arrival(ref, rsem):
        rcopy(ref, ref, s_y.at[0], rsem, torus=mate).wait_recv()

    late = []

    def sent(copy, when=None):
        copy.start()
        late.append((when, copy))

    lane0 = pl.multiple_of(c * width, 128)

    own_w = (
        (gate_hbm, w_gate.at[pl.ds(lane0, width), :]),
        (up_hbm, w_up.at[pl.ds(lane0, width), :]),
        (down_hbm, w_down.at[c]),
    )
    loads = [pltpu.make_async_copy(src, dst, s_w.at[i]) for i, (src, dst) in enumerate(own_w)]
    for load in loads:
        load.start()

    barrier = pltpu.get_barrier_semaphore()
    greeted = 0
    for step in range(1, n_node):
        for core in range(2):
            pl.semaphore_signal(barrier, 1, device_id={"node": (z + step) % n_node, "torus": x * 2 + core}, device_id_type=MESH)
            greeted += 1
    for step in range(1, n_torus):
        pl.semaphore_signal(barrier, 1, device_id={"torus": (t + step) % n_torus}, device_id_type=MESH)
        greeted += 1
    if n_section > 1:
        @pl.when(sec > 0)
        def _():
            pl.semaphore_signal(barrier, 1, device_id={"section": sec - 1}, device_id_type=MESH)

    def routing_key(tick):
        ids = lax.broadcasted_iota(jnp.int32, (16, tokens), 0)
        hit = jnp.zeros((16, tokens), jnp.bool_)
        for k in range(lanes_e.shape[1]):
            rel = (lanes_e[tick, k : k + 1, :] - z + n_node) % n_node
            hit = hit | (rel == ids)
        before = lax.broadcasted_iota(jnp.int32, (tokens, tokens), 0) < lax.broadcasted_iota(jnp.int32, (tokens, tokens), 1)
        rank = dot(hit.astype(F32).astype(BF16), before.astype(F32).astype(BF16))
        return jnp.where(hit, rank, -1.0)

    def combine_table(tick):
        lane = lax.broadcasted_iota(jnp.int32, (tokens, 128), 1)
        after = lax.broadcasted_iota(jnp.int32, (tokens, tokens), 1) < lax.broadcasted_iota(jnp.int32, (tokens, tokens), 0)
        marks = []
        for k in range(rows_e.shape[2]):
            rel = (rows_e[tick, :, k : k + 1] - z + n_node) % n_node
            marks.append(rel == lane)
        hit = functools.reduce(jnp.logical_or, marks)
        rank = dot(after.astype(F32).astype(BF16), hit.astype(F32).astype(BF16))
        place = rank + lane.astype(F32) * capacity
        slot = lax.broadcasted_iota(jnp.int32, (tokens, n_node * capacity), 1).astype(F32)
        table = jnp.zeros((tokens, n_node * capacity), F32)
        for k, mark in enumerate(marks):
            target = jnp.sum(jnp.where(mark, place, 0.0), axis=1, keepdims=True)
            table = table + jnp.where(slot == target, rows_w[tick, :, k : k + 1], 0.0)
        high = table.astype(BF16)
        combine_w[tick, 0] = high
        combine_w[tick, 1] = (table - high.astype(F32)).astype(BF16)

    def quantize(stream, scale):
        value = stream.astype(F32) * (FP8_LIMIT / scale)
        quant[...] = jnp.clip(value, -FP8_LIMIT, FP8_LIMIT).astype(BF16)

    def peak_begin(tick, stream):
        pk_src[tick, 0] = jnp.full((8, 128), jnp.max(jnp.abs(stream.astype(F32))), F32)
        for step in range(1, n_node):
            sent(rcopy(pk_src.at[tick, 0], pk_node.at[tick, step], s_pn.at[tick, step], r_pn.at[tick, step], node=(z + step) % n_node))

    def peak_middle(tick):
        top = pk_src[tick, 0]
        for step in range(1, n_node):
            arrival(pk_node.at[tick, step], r_pn.at[tick, step])
            top = jnp.maximum(top, pk_node[tick, step])
        pk_src[tick, 1] = top
        for step in range(1, n_torus):
            sent(rcopy(pk_src.at[tick, 1], pk_torus.at[tick, step], s_pt.at[tick, step], r_pt.at[tick, step], torus=(t + step) % n_torus))

    def peak_end(tick):
        top = pk_src[tick, 1]
        for step in range(1, n_torus):
            arrival(pk_torus.at[tick, step], r_pt.at[tick, step])
            top = jnp.maximum(top, pk_torus[tick, step])
        return jnp.max(top)

    order = [(-core_rel[core][k]) % n_node for k in range(n_step) for core in range(2)]

    def dispatch(tick, key):
        rank_row = lax.broadcasted_iota(jnp.int32, (capacity, tokens), 0).astype(F32)
        for step in order:
            pick = (rank_row == key[step : step + 1, :]).astype(F32).astype(BF16)
            block = dot(pick, quant[...]).astype(BF16)
            core, k = where_rel[(-step) % n_node]
            target = arrived.at[tick, k, :, pl.ds(lane0, width)]
            if step:
                d_send[tick, step] = block
                sent(rcopy(d_send.at[tick, step], target, s_d.at[tick, step], r_d.at[tick, k, c], node=(z + step) % n_node, torus=x * 2 + core))
            else:
                @pl.when(c == core)
                def _():
                    arrived[tick, k, :, core * width : (core + 1) * width] = block

                @pl.when(c != core)
                def _():
                    d_send[tick, step] = block
                    rcopy(d_send.at[tick, step], target, s_d.at[tick, step], r_d.at[tick, k, c], torus=mate).start()

                late.append((c != core, rcopy(d_send.at[tick, step], target, s_d.at[tick, step], r_d.at[tick, k, c], torus=mate)))

    def stage_gate(tick, k):
        for half in range(2):
            def wait(half=half):
                arrival(arrived.at[tick, k, :, pl.ds(half * width, width)], r_d.at[tick, k, half])

            if where_rel[0] == (half, k):
                pl.when(c != half)(wait)
            else:
                wait()

        def body(j, carry):
            block = (x + 1 + j) % n_x
            cols = pl.ds(pl.multiple_of(block * unit, 128), unit)
            gate = dot(arrived[tick, k], w_gate[:, cols])
            up = dot(arrived[tick, k], w_up[:, cols])

            @pl.when(j < n_x - 1)
            def _():
                rs_send[tick, k, j, :, :unit] = gate.astype(BF16)
                rs_send[tick, k, j, :, unit:] = up.astype(BF16)
                rcopy(rs_send.at[tick, k, j], rs_recv.at[tick, k, j], s_rs.at[tick, k, j], r_rs.at[tick, k, j], torus=block * 2 + c).start()

            @pl.when(j == n_x - 1)
            def _():
                own_part[k, :, :unit] = gate
                own_part[k, :, unit:] = up

            return carry

        lax.fori_loop(0, n_x, body, 0)
        for j in range(n_x - 1):
            late.append((None, rcopy(rs_send.at[tick, k, j], rs_recv.at[tick, k, j], s_rs.at[tick, k, j], r_rs.at[tick, k, j], torus=((x + 1 + j) % n_x) * 2 + c)))

    def stage_hidden(tick, k, dequant):
        total = own_part[k]
        for j in range(n_x - 1):
            arrival(rs_recv.at[tick, k, j], r_rs.at[tick, k, j])
            total = total + rs_recv[tick, k, j].astype(F32)
        gate = total[:, :unit] * dequant
        up = total[:, unit:] * dequant
        cols = pl.ds(pl.multiple_of(x * unit, 128), unit)
        hidden[tick, k, :, cols] = (gate / (1.0 + jnp.exp(-gate)) * up).astype(BF16)
        for j in range(n_x - 1):
            place = hidden.at[tick, k, :, cols]
            sent(rcopy(place, place, s_h.at[tick, k, j], r_h.at[tick, k, j], torus=((x + 1 + j) % n_x) * 2 + c))

    def stage_down(tick, k):
        for j in range(n_x - 1):
            source = (x + 2 * n_x - 1 - j) % n_x
            arrival(hidden.at[tick, k, :, pl.ds(pl.multiple_of(source * unit, 128), unit)], r_h.at[tick, k, j])
        rel = jnp.where(c == 0, core_rel[0][k], core_rel[1][k])
        home = (z + rel) % n_node
        place = (n_node - rel) % n_node
        target = results.at[tick, pl.ds(pl.multiple_of(place * capacity, 16), capacity), :]
        core0, k0 = where_rel[0]
        for half in range(2):
            value = dot(hidden[tick, k], w_down[half]).astype(BF16)
            copy = rcopy(r_send.at[tick, k, half], target, s_r.at[tick, k, half], r_r.at[tick, place], node=home, torus=x * 2 + half)
            if k == k0 and half == core0:
                @pl.when(c == core0)
                def _():
                    results[tick, 0:capacity, :] = value

                @pl.when(c != core0)
                def _():
                    r_send[tick, k, half] = value
                    copy.start()

                late.append((c != core0, copy))
            else:
                r_send[tick, k, half] = value
                sent(copy)

    def stage_combine(tick, stream):
        core0, _k0 = where_rel[0]
        for place in range(n_node):
            def wait(place=place):
                arrival(results.at[tick, pl.ds(place * capacity, capacity), :], r_r.at[tick, place])

            if place == 0:
                pl.when(c != core0)(wait)
            else:
                wait()
        branch = dot(combine_w[tick, 0], results[tick]) + dot(combine_w[tick, 1], results[tick])
        out[tick] = (stream.astype(F32) + branch).astype(BF16)

    scale = hist[0]
    quantize(act[...], scale)
    key = routing_key(0)
    pl.semaphore_wait(barrier, greeted + jnp.where(sec < n_section - 1, 1, 0))
    dispatch(0, key)
    for i, load in enumerate(loads):
        load.wait()
        src, dst = own_w[i]
        sent(rcopy(dst, dst, s_wp.at[i], r_wp.at[i], torus=mate))
    peak_begin(0, act[...])
    combine_table(0)
    combine_table(1)

    schedule = []
    for k in range(n_step):
        schedule.append(("gate", k))
        if k >= 1:
            schedule.append(("hidden", k - 1))
        if k >= 2:
            schedule.append(("down", k - 2))
    schedule.append(("hidden", n_step - 1))
    if n_step >= 2:
        schedule.append(("down", n_step - 2))
    schedule.append(("down", n_step - 1))

    other = (
        w_gate.at[pl.ds(pl.multiple_of((1 - c) * width, 128), width), :],
        w_up.at[pl.ds(pl.multiple_of((1 - c) * width, 128), width), :],
        w_down.at[1 - c],
    )

    for tick in range(ticks):
        stream = act if tick == 0 else y_buf
        dequant = scale / FP8_LIMIT
        for kind, k in schedule:
            if kind == "gate":
                if tick == 0 and k == 0:
                    arrival(other[0], r_wp.at[0])
                    arrival(other[1], r_wp.at[1])
                stage_gate(tick, k)
                if k == 0:
                    peak_middle(tick)
            elif kind == "hidden":
                stage_hidden(tick, k, dequant)
            else:
                if tick == 0 and k == 0:
                    arrival(other[2], r_wp.at[2])
                stage_down(tick, k)
        peak = peak_end(tick)
        peak_out[0, tick] = peak
        stage_combine(tick, stream[...])
        if tick + 1 < ticks:
            scale = peak
            key = routing_key(tick + 1)
            if n_section > 1:
                @pl.when(sec < n_section - 1)
                def _():
                    rcopy(out.at[tick], y_buf, s_y.at[0], r_y.at[0], section=sec + 1).start()

                late.append((sec < n_section - 1, rcopy(out.at[tick], y_buf, s_y.at[0], r_y.at[0], section=sec + 1)))

                @pl.when(sec > 0)
                def _():
                    rcopy(out.at[tick], y_buf, s_y.at[0], r_y.at[0], section=sec - 1).wait_recv()

            @pl.when(sec == 0)
            def _():
                y_buf[...] = nxt[...]

            quantize(y_buf[...], scale)
            dispatch(tick + 1, key)
            peak_begin(tick + 1, y_buf[...])

    for when, copy in late:
        if when is None:
            copy.wait_send()
        else:
            pl.when(when)(copy.wait_send)


def solution(mesh):
    n_section, n_node, n_torus = (mesh.shape[a] for a in ("section", "node", "torus"))
    n_x = n_torus // 2

    def shards(act_in, next_in, routes, route_w, hist, gate_w, up_w, down_w):
        tokens, width = next_in.shape
        ticks, _, _, top = routes.shape
        capacity = 5 * tokens * top // (4 * n_node)
        ffw = gate_w.shape[3]
        unit = ffw // n_x
        n_step = n_node // 2
        lanes_e = routes[:, 0].transpose(0, 2, 1)
        rows_e = routes[:, 0]
        rows_w = route_w[:, 0]
        vmem = pl.BlockSpec(memory_space=pltpu.VMEM)
        hbm = pl.BlockSpec(memory_space=pl.ANY)
        smem = pl.BlockSpec(memory_space=pltpu.SMEM)
        dma = pltpu.SemaphoreType.DMA
        out, peak = pl.pallas_call(
            functools.partial(kernel, n_section, n_node, n_torus, capacity),
            out_shape=(
                jax.ShapeDtypeStruct((ticks, tokens, width), BF16),
                jax.ShapeDtypeStruct((1, ticks), F32),
            ),
            in_specs=[vmem, vmem, vmem, vmem, vmem, smem, hbm, hbm, hbm],
            out_specs=(vmem, smem),
            scratch_shapes=[
                pltpu.VMEM((2 * width, ffw), BF16),
                pltpu.VMEM((2 * width, ffw), BF16),
                pltpu.VMEM((2, ffw, width), BF16),
                pltpu.VMEM((tokens, width), BF16),
                pltpu.VMEM((ticks, n_node, capacity, width), BF16),
                pltpu.VMEM((ticks, n_step, capacity, 2 * width), BF16),
                pltpu.VMEM((n_step, capacity, 2 * unit), F32),
                pltpu.VMEM((ticks, n_step, max(1, n_x - 1), capacity, 2 * unit), BF16),
                pltpu.VMEM((ticks, n_step, max(1, n_x - 1), capacity, 2 * unit), BF16),
                pltpu.VMEM((ticks, n_step, capacity, ffw), BF16),
                pltpu.VMEM((ticks, n_step, 2, capacity, width), BF16),
                pltpu.VMEM((ticks, n_node * capacity, width), BF16),
                pltpu.VMEM((ticks, 2, tokens, n_node * capacity), BF16),
                pltpu.VMEM((tokens, width), BF16),
                pltpu.VMEM((ticks, 2, 8, 128), F32),
                pltpu.VMEM((ticks, n_node, 8, 128), F32),
                pltpu.VMEM((ticks, n_torus, 8, 128), F32),
                dma((3,)), dma((3,)), dma((3,)),
                dma((ticks, n_node)), dma((ticks, n_step, 2)),
                dma((ticks, n_step, max(1, n_x - 1))), dma((ticks, n_step, max(1, n_x - 1))),
                dma((ticks, n_step, max(1, n_x - 1))), dma((ticks, n_step, max(1, n_x - 1))),
                dma((ticks, n_step, 2)), dma((ticks, n_node)),
                dma((1,)), dma((1,)),
                dma((ticks, n_node)), dma((ticks, n_node)),
                dma((ticks, n_torus)), dma((ticks, n_torus)),
            ],
            compiler_params=pltpu.CompilerParams(collective_id=0, has_side_effects=True),
        )(act_in[0], next_in, lanes_e, rows_e, rows_w, hist, gate_w[0, 0], up_w[0, 0], down_w[0, 0])
        return out[:, None], peak

    return jax.shard_map(
        shards,
        mesh=mesh,
        in_specs=(
            P("section", "node", "torus"),
            P("node", "torus"),
            P(None, "section", "node", None),
            P(None, "section", "node", None),
            P("section"),
            P("section", "node", "torus", None),
            P("section", "node", "torus", None),
            P("section", "node", None, "torus"),
        ),
        out_specs=(P(None, "section", "node", "torus"), P("section", None)),
        check_vma=False,
    )
```

```python
import functools

import jax
import jax.numpy as jnp
from jax import lax
from jax.experimental import pallas as pl
from jax.experimental.pallas import tpu as pltpu
from jax.sharding import PartitionSpec as P

MESH = pl.DeviceIdType.MESH
FP8_LIMIT = 448.0
F32 = jnp.float32
BF16 = jnp.bfloat16


PARTS = 3
LAG = 1
ORDER = (("gate", 0), ("gate", 1), ("hidden", 0), ("gate", 2), ("hidden", 1), ("down", 0),
         ("gate", 3), ("down", 1), ("hidden", 2), ("hidden", 3), ("down", 2), ("down", 3))
SCHEDULES = (ORDER, ORDER)


def PLAN(piece, places):
    if PARTS < 3 or len(places) < 8:
        return [(piece, places)]
    if piece == 0:
        return [(0, places)]
    if piece == 1:
        return [(1, places[:4])]
    return [(2, places[:4]), (1, places[4:6]), (2, places[4:6]), (1, places[6:]), (2, places[6:])]


def source_tables(n_node):
    if n_node == 8:
        return ((0, 1, 6, 3), (7, 2, 5, 4))
    half = n_node // 2
    return (tuple(range(half)), tuple(range(half, n_node)))


def column_cuts(width, parts):
    unit = width // 128
    parts = min(parts, unit)
    edges = [unit * i // parts * 128 for i in range(parts + 1)]
    return list(zip(edges, edges[1:]))


def dot(a, b):
    return jnp.dot(a, b, preferred_element_type=F32)


def kernel(
    n_section, n_node, n_torus, capacity,
    act, nxt, lanes_e, lanes_w, hist, gate_hbm, up_hbm, down_hbm,
    out, peak_out,
    w_gate, w_up, w_down, quant, d_send, arrived, own_part, rs_send, rs_recv,
    hidden, r_send, results, early_w, late_w, total_buf, y_buf, pk_src, pk_node, pk_torus,
    s_w, s_wp, r_wp, s_d, r_d, s_rs, r_rs, s_h, r_h, s_r, r_r, s_y, r_y, s_pn, r_pn, s_pt, r_pt,
):
    ticks, tokens, width = out.shape
    n_x = n_torus // 2
    ffw = w_gate.shape[1]
    unit = ffw // n_x
    core_rel = source_tables(n_node)
    n_step = len(core_rel[0])
    where_rel = {rel: (c, k) for c in range(2) for k, rel in enumerate(core_rel[c])}
    last = n_step - 1
    cuts = column_cuts(width, PARTS)
    places = [(-core_rel[core][k]) % n_node for k in range(n_step) for core in range(2)]
    position = {place: i for i, place in enumerate(places)}
    n_early = 2 * last
    whole = (0, width)

    sec = lax.axis_index("section")
    z = lax.axis_index("node")
    t = lax.axis_index("torus")
    x = t // 2
    c = t % 2
    mate = x * 2 + (1 - c)

    def rcopy(src, dst, ssem, rsem, node=None, torus=None, section=None):
        ids = {}
        if section is not None:
            ids["section"] = section
        if node is not None:
            ids["node"] = node
        if torus is not None:
            ids["torus"] = torus
        return pltpu.make_async_remote_copy(src, dst, ssem, rsem, device_id=ids, device_id_type=MESH)

    def arrival(ref, rsem):
        with jax.named_scope("wait"):
            rcopy(ref, ref, s_y.at[0], rsem, torus=mate).wait_recv()

    late = []

    def gone(ref, ssem, when=None):
        late.append((when, rcopy(ref, ref, ssem, r_y.at[0], torus=mate)))

    lane0 = pl.multiple_of(c * width, 128)

    own_w = (
        (gate_hbm, w_gate.at[pl.ds(lane0, width), :]),
        (up_hbm, w_up.at[pl.ds(lane0, width), :]),
        (down_hbm, w_down.at[c]),
    )
    loads = [pltpu.make_async_copy(src, dst, s_w.at[i]) for i, (src, dst) in enumerate(own_w)]
    for load in loads:
        load.start()

    barrier = pltpu.get_barrier_semaphore()
    greeted = 0
    for step in range(1, n_node):
        for core in range(2):
            pl.semaphore_signal(barrier, 1, device_id={"node": (z + step) % n_node, "torus": x * 2 + core}, device_id_type=MESH)
            greeted += 1
    for step in range(1, n_torus):
        pl.semaphore_signal(barrier, 1, device_id={"torus": (t + step) % n_torus}, device_id_type=MESH)
        greeted += 1
    if n_section > 1:
        @pl.when(sec > 0)
        def _():
            pl.semaphore_signal(barrier, 1, device_id={"section": sec - 1}, device_id_type=MESH)

    def routing_key(tick):
        ids = lax.broadcasted_iota(jnp.int32, (16, tokens), 0)
        hit = jnp.zeros((16, tokens), jnp.bool_)
        for k in range(lanes_e.shape[1]):
            rel = (lanes_e[tick, k : k + 1, :] - z + n_node) % n_node
            hit = hit | (rel == ids)
        before = lax.broadcasted_iota(jnp.int32, (tokens, tokens), 0) < lax.broadcasted_iota(jnp.int32, (tokens, tokens), 1)
        rank = dot(hit.astype(F32).astype(BF16), before.astype(F32).astype(BF16))
        return jnp.where(hit, rank, -1.0)

    def combine_table(tick):
        lane = lax.broadcasted_iota(jnp.int32, (tokens, 128), 1)
        after = lax.broadcasted_iota(jnp.int32, (tokens, tokens), 1) < lax.broadcasted_iota(jnp.int32, (tokens, tokens), 0)
        top = lanes_e.shape[1]
        rel = ((lanes_e[tick] - z + n_node) % n_node).astype(F32)
        rows = jnp.concatenate([rel, lanes_w[tick], jnp.zeros((128 - 2 * top, tokens), F32)], axis=0)
        turned = rows.T
        marks = [turned[:, k : k + 1] == lane.astype(F32) for k in range(top)]
        hit = functools.reduce(jnp.logical_or, marks)
        spot = dot(after.astype(F32).astype(BF16), hit.astype(F32).astype(BF16))
        for place, at in position.items():
            spot = spot + jnp.where(lane == place, F32(at * capacity), 0.0)
        slot = lax.broadcasted_iota(jnp.int32, (tokens, n_node * capacity), 1).astype(F32)
        table = jnp.zeros((tokens, n_node * capacity), F32)
        for k, mark in enumerate(marks):
            target = jnp.sum(jnp.where(mark, spot, 0.0), axis=1, keepdims=True)
            table = table + jnp.where(slot == target, turned[:, top + k : top + k + 1], 0.0)
        high = table.astype(BF16)
        low = (table - high.astype(F32)).astype(BF16)
        edge = n_early * capacity
        for i, part in enumerate((high, low)):
            early_w[tick, i] = part[:, :edge]
            late_w[tick, i] = part[:, edge:]

    def quantize(stream, scale, span):
        value = stream[:, span[0] : span[1]].astype(F32) * (FP8_LIMIT / scale)
        quant[:, span[0] : span[1]] = jnp.clip(value, -FP8_LIMIT, FP8_LIMIT).astype(BF16)

    def peak_begin(tick, stream):
        pk_src[tick, 0] = jnp.full((8, 128), jnp.max(jnp.abs(stream.astype(F32))), F32)
        for step in range(1, n_node):
            rcopy(pk_src.at[tick, 0], pk_node.at[tick, step], s_pn.at[tick], r_pn.at[tick], node=(z + step) % n_node).start()
        gone(pk_node.at[tick, 1:], s_pn.at[tick])

    def peak_middle(tick):
        top = pk_src[tick, 0]
        arrival(pk_node.at[tick, 1:], r_pn.at[tick])
        for step in range(1, n_node):
            top = jnp.maximum(top, pk_node[tick, step])
        pk_src[tick, 1] = top
        for step in range(1, n_torus):
            rcopy(pk_src.at[tick, 1], pk_torus.at[tick, step], s_pt.at[tick], r_pt.at[tick], torus=(t + step) % n_torus).start()
        gone(pk_torus.at[tick, 1:], s_pt.at[tick])

    def peak_end(tick):
        top = pk_src[tick, 1]
        arrival(pk_torus.at[tick, 1:], r_pt.at[tick])
        for step in range(1, n_torus):
            top = jnp.maximum(top, pk_torus[tick, step])
        return jnp.max(top)

    def spans_of_dispatch(tick):
        return [whole] if tick == 0 else cuts

    def spans_of_return(tick, k):
        return cuts if k == last and tick + 1 < ticks else [whole]

    def dispatch(tick, key, piece, steps=places):
        a, b = spans_of_dispatch(tick)[piece]
        rank_row = lax.broadcasted_iota(jnp.int32, (capacity, tokens), 0).astype(F32)
        for step in steps:
            pick = (rank_row == key[step : step + 1, :]).astype(F32).astype(BF16)
            block = dot(pick, quant[:, a:b]).astype(BF16)
            core, k = where_rel[(-step) % n_node]
            copy = rcopy(
                d_send.at[tick, step, :, a:b],
                arrived.at[tick, k, :, pl.ds(pl.multiple_of(lane0 + a, 128), b - a)],
                s_d.at[tick, 0 if step else 1], r_d.at[tick, k, c],
                node=(z + step) % n_node, torus=x * 2 + core if step else mate,
            )
            if step:
                d_send[tick, step, :, a:b] = block
                copy.start()
            else:
                @pl.when(c == core)
                def _():
                    arrived[tick, k, :, core * width + a : core * width + b] = block

                @pl.when(c != core)
                def _():
                    d_send[tick, step, :, a:b] = block
                    copy.start()

    def stage_gate(tick, k):
        if k == 0:
            gone(d_send.at[tick, 1:], s_d.at[tick, 0])
            gone(d_send.at[tick, 0], s_d.at[tick, 1], c != where_rel[0][0])
        for half in range(2):
            def wait(half=half):
                arrival(arrived.at[tick, k, :, half * width : (half + 1) * width], r_d.at[tick, k, half])

            if where_rel[0] == (half, k):
                pl.when(c != half)(wait)
            else:
                wait()

        def body(j, carry):
            block = (x + 1 + j) % n_x
            cols = pl.ds(pl.multiple_of(block * unit, 128), unit)
            gate = dot(arrived[tick, k], w_gate[:, cols])
            up = dot(arrived[tick, k], w_up[:, cols])

            @pl.when(j < n_x - 1)
            def _():
                rs_send[tick, k, j, :, :unit] = gate.astype(BF16)
                rs_send[tick, k, j, :, unit:] = up.astype(BF16)
                rcopy(rs_send.at[tick, k, j], rs_recv.at[tick, k, j], s_rs.at[tick], r_rs.at[tick, k], torus=block * 2 + c).start()

            @pl.when(j == n_x - 1)
            def _():
                own_part[k, :, :unit] = gate
                own_part[k, :, unit:] = up

            return carry

        with jax.named_scope(f"gatemm{tick}{k}"):
            lax.fori_loop(0, n_x, body, 0)
        if k == last and n_x > 1:
            gone(rs_send.at[tick], s_rs.at[tick])

    def stage_hidden(tick, k, dequant):
        total = own_part[k]
        if n_x > 1:
            arrival(rs_recv.at[tick, k], r_rs.at[tick, k])
        for j in range(n_x - 1):
            total = total + rs_recv[tick, k, j].astype(F32)
        gate = total[:, :unit] * dequant
        up = total[:, unit:] * dequant
        cols = pl.ds(pl.multiple_of(x * unit, 128), unit)
        hidden[tick, k, :, cols] = (gate / (1.0 + jnp.exp(-gate)) * up).astype(BF16)
        for j in range(n_x - 1):
            place = hidden.at[tick, k, :, cols]
            rcopy(place, place, s_h.at[tick], r_h.at[tick, k], torus=((x + 1 + j) % n_x) * 2 + c).start()
        if k == last and n_x > 1:
            gone(hidden.at[tick, :, :, : (n_x - 1) * unit], s_h.at[tick])

    def stage_down(tick, k):
        if n_x > 1:
            arrival(hidden.at[tick, k, :, : (n_x - 1) * unit], r_h.at[tick, k])
        home = (z + jnp.where(c == 0, core_rel[0][k], core_rel[1][k])) % n_node
        at = 2 * k + c
        core0, k0 = where_rel[0]
        spans = spans_of_return(tick, k)
        for piece, (a, b) in enumerate(spans):
            for half in range(2):
                value = dot(hidden[tick, k], w_down[half, :, a:b]).astype(BF16)
                own = k == k0 and half == core0
                if k == last:
                    ssem, rsem = s_r.at[tick, 2 + piece], r_r.at[tick, 2 + piece]
                else:
                    ssem = s_r.at[tick, 1 if own else 0]
                    rsem = r_r.at[tick, jnp.where(c == core0, 1, 0) if k == k0 else 0]
                copy = rcopy(
                    r_send.at[tick, k, half, :, a:b],
                    results.at[tick, pl.ds(pl.multiple_of(at * capacity, 16), capacity), a:b],
                    ssem, rsem, node=home, torus=x * 2 + half,
                )
                if own:
                    @pl.when(c == core0)
                    def _():
                        results[tick, 0:capacity, a:b] = value

                    @pl.when(c != core0)
                    def _():
                        r_send[tick, k, half, :, a:b] = value
                        copy.start()
                else:
                    r_send[tick, k, half, :, a:b] = value
                    copy.start()
            if k == last:
                gone(r_send.at[tick, k, :, :, a:b], s_r.at[tick, 2 + piece])
                if piece + 1 < len(spans):
                    late.pop()[1].wait_send()
        if k == last:
            gone(d_send.at[tick, : n_early - 1], s_r.at[tick, 0])
            gone(r_send.at[tick, k0, core0], s_r.at[tick, 1], c != core0)

    def results_in(tick, piece=None):
        if piece is None:
            arrival(results.at[tick, capacity : n_early * capacity, :], r_r.at[tick, 0])

            @pl.when(c != where_rel[0][0])
            def _():
                arrival(results.at[tick, 0:capacity, :], r_r.at[tick, 1])
        else:
            a, b = spans_of_return(tick, last)[piece]
            arrival(results.at[tick, n_early * capacity :, a:b], r_r.at[tick, 2 + piece])

    def combine_early(tick, stream):
        results_in(tick)
        rows = results[tick, : n_early * capacity, :]
        total_buf[...] = stream.astype(F32) + dot(early_w[tick, 0], rows) + dot(early_w[tick, 1], rows)

    def combine_late(tick, piece):
        a, b = spans_of_return(tick, last)[piece]
        results_in(tick, piece)
        rows = results[tick, n_early * capacity :, a:b]
        total = total_buf[:, a:b] + dot(late_w[tick, 0], rows) + dot(late_w[tick, 1], rows)
        out[tick, :, a:b] = total.astype(BF16)

    def relay(tick, piece):
        a, b = cuts[piece]
        return rcopy(out.at[tick, :, a:b], y_buf.at[:, a:b], s_y.at[0], r_y.at[piece], section=(sec + 1) % n_section)

    scale = hist[0]
    with jax.named_scope("start"):
        quantize(act, scale, whole)
        key = routing_key(0)
    with jax.named_scope("bar"):
      pl.semaphore_wait(barrier, greeted + jnp.where(sec < n_section - 1, 1, 0))
    peak_begin(0, act[...])
    with jax.named_scope("disp0"):
        dispatch(0, key, 0)
    for i, load in enumerate(loads):
        load.wait()
        src, dst = own_w[i]
        rcopy(dst, dst, s_wp.at[i], r_wp.at[i], torus=mate).start()
        gone(dst, s_wp.at[i])
    with jax.named_scope("tables"):
        combine_table(0)
        combine_table(1)

    def schedule_of(tick):
        if n_step == 4:
            return SCHEDULES[tick]
        return [(kind, k) for k in range(n_step) for kind in ("gate", "hidden", "down")]

    other = (
        w_gate.at[pl.ds(pl.multiple_of((1 - c) * width, 128), width), :],
        w_up.at[pl.ds(pl.multiple_of((1 - c) * width, 128), width), :],
        w_down.at[1 - c],
    )

    for tick in range(ticks):
        stream = act if tick == 0 else y_buf
        dequant = scale / FP8_LIMIT
        for kind, k in schedule_of(tick):
          with jax.named_scope(f"{kind}{tick}{k}"):
            if kind == "gate":
                if tick == 0 and k == 0:
                    arrival(other[0], r_wp.at[0])
                    arrival(other[1], r_wp.at[1])
                stage_gate(tick, k)
                if tick == 0 and k == last:
                    peak_middle(tick)
            elif kind == "hidden":
                stage_hidden(tick, k, dequant)
                if tick > 0 and k == last:
                    peak_middle(tick)
            else:
                if tick == 0 and k == 0:
                    arrival(other[2], r_wp.at[2])
                stage_down(tick, k)
        with jax.named_scope(f"peakend{tick}"):
            peak = peak_end(tick)
            peak_out[0, tick] = peak
        with jax.named_scope(f"early{tick}"):
            combine_early(tick, stream[...])
        if tick + 1 == ticks:
            with jax.named_scope(f"late{tick}"):
                combine_late(tick, 0)
            continue
        scale = peak
        key = routing_key(tick + 1)

        def pass_on(piece):
            with jax.named_scope(f"late{tick}{piece}"):
                combine_late(tick, piece)
            if n_section > 1:
                pl.when(sec < n_section - 1)(relay(tick, piece).start)

        def take_up(piece):
            a, b = cuts[piece]
            with jax.named_scope(f"waity{piece}"):
                if n_section > 1:
                    pl.when(sec > 0)(relay(tick, piece).wait_recv)

                @pl.when(sec == 0)
                def _():
                    y_buf[:, a:b] = nxt[:, a:b]

            with jax.named_scope(f"disp{piece}"):
                quantize(y_buf, scale, (a, b))
                for p, steps in PLAN(piece, places):
                    dispatch(tick + 1, key, p, steps)

        if n_section > 1:
            gone(out.at[tick], s_y.at[0], sec < n_section - 1)
        for piece in range(len(cuts)):
            pass_on(piece)
            if piece >= LAG:
                take_up(piece - LAG)
        for piece in range(max(0, len(cuts) - LAG), len(cuts)):
            take_up(piece)
        peak_begin(tick + 1, y_buf[...])

    with jax.named_scope("tail"):
        for when, copy in late:
            if when is None:
                copy.wait_send()
            else:
                pl.when(when)(copy.wait_send)


def solution(mesh):
    n_section, n_node, n_torus = (mesh.shape[a] for a in ("section", "node", "torus"))
    n_x = n_torus // 2

    def shards(act_in, next_in, routes, route_w, hist, gate_w, up_w, down_w):
        tokens, width = next_in.shape
        ticks, _, _, top = routes.shape
        capacity = 5 * tokens * top // (4 * n_node)
        ffw = gate_w.shape[3]
        unit = ffw // n_x
        n_step = n_node // 2
        lanes_e = routes[:, 0].transpose(0, 2, 1)
        lanes_w = route_w[:, 0].transpose(0, 2, 1)
        late_rows = 2 * capacity
        early_rows = (n_step - 1) * late_rows
        parts = len(column_cuts(width, PARTS))
        vmem = pl.BlockSpec(memory_space=pltpu.VMEM)
        hbm = pl.BlockSpec(memory_space=pl.ANY)
        smem = pl.BlockSpec(memory_space=pltpu.SMEM)
        dma = pltpu.SemaphoreType.DMA
        out, peak = pl.pallas_call(
            functools.partial(kernel, n_section, n_node, n_torus, capacity),
            out_shape=(
                jax.ShapeDtypeStruct((ticks, tokens, width), BF16),
                jax.ShapeDtypeStruct((1, ticks), F32),
            ),
            in_specs=[vmem, vmem, vmem, vmem, smem, hbm, hbm, hbm],
            out_specs=(vmem, smem),
            scratch_shapes=[
                pltpu.VMEM((2 * width, ffw), BF16),
                pltpu.VMEM((2 * width, ffw), BF16),
                pltpu.VMEM((2, ffw, width), BF16),
                pltpu.VMEM((tokens, width), BF16),
                pltpu.VMEM((ticks, n_node, capacity, width), BF16),
                pltpu.VMEM((ticks, n_step, capacity, 2 * width), BF16),
                pltpu.VMEM((n_step, capacity, 2 * unit), F32),
                pltpu.VMEM((ticks, n_step, max(1, n_x - 1), capacity, 2 * unit), BF16),
                pltpu.VMEM((ticks, n_step, max(1, n_x - 1), capacity, 2 * unit), BF16),
                pltpu.VMEM((ticks, n_step, capacity, ffw), BF16),
                pltpu.VMEM((ticks, n_step, 2, capacity, width), BF16),
                pltpu.VMEM((ticks, n_node * capacity, width), BF16),
                pltpu.VMEM((ticks, 2, tokens, early_rows), BF16),
                pltpu.VMEM((ticks, 2, tokens, late_rows), BF16),
                pltpu.VMEM((tokens, width), F32),
                pltpu.VMEM((tokens, width), BF16),
                pltpu.VMEM((ticks, 2, 8, 128), F32),
                pltpu.VMEM((ticks, n_node, 8, 128), F32),
                pltpu.VMEM((ticks, n_torus, 8, 128), F32),
                dma((3,)), dma((3,)), dma((3,)),
                dma((ticks, 2)), dma((ticks, n_step, 2)),
                dma((ticks,)), dma((ticks, n_step)),
                dma((ticks,)), dma((ticks, n_step)),
                dma((ticks, 2 + parts)), dma((ticks, 2 + parts)),
                dma((1,)), dma((parts,)),
                dma((ticks,)), dma((ticks,)), dma((ticks,)), dma((ticks,)),
            ],
            compiler_params=pltpu.CompilerParams(collective_id=0, has_side_effects=True),
        )(act_in[0], next_in, lanes_e, lanes_w, hist, gate_w[0, 0], up_w[0, 0], down_w[0, 0])
        return out[:, None], peak

    return jax.shard_map(
        shards,
        mesh=mesh,
        in_specs=(
            P("section", "node", "torus"),
            P("node", "torus"),
            P(None, "section", "node", None),
            P(None, "section", "node", None),
            P("section"),
            P("section", "node", "torus", None),
            P("section", "node", "torus", None),
            P("section", "node", None, "torus"),
        ),
        out_specs=(P(None, "section", "node", "torus"), P("section", None)),
        check_vma=False,
    )
```
